1024 devices in a mesh: expert: 8 (over x), dp: 8 (over z_lo, core), mp: 16 (over z_hi, y).
Axes of the slice: x: 8, y: 8, z: 8 (z_hi: 2, z_lo: 4; z = z_hi * 4 + z_lo), core: 2. Of those that a mesh axis runs over, the one named last changes fastest.
Arguments:
- tokens: bfloat16 [768, 4096], P(('expert', 'dp'), 'mp'), may hold values from -6 to 6
- routes: int32 [768, 2], P(('expert', 'dp')), may hold values from 0 to 7, all different within a row; in each aligned block of 12 rows (0 to 11, 12 to 23, ...) at most 5 rows name the same one
- router_weight: bfloat16 [4096, 8], P('mp'), may hold values from -0.09375 to 0.09375
- gate_weight: bfloat16 [8, 4096, 16384], P('expert', None, ('dp', 'mp')), may hold values from -0.09375 to 0.09375
- up_weight: bfloat16 [8, 4096, 16384], P('expert', None, ('dp', 'mp')), may hold values from -0.09375 to 0.09375
- down_weight: bfloat16 [8, 16384, 4096], P('expert', ('dp', 'mp')), may hold values from -0.1875 to 0.1875
Outputs:
- mixed: bfloat16 [768, 4096], P(('expert', 'dp'), 'mp')
The draws below stay inside these ranges and needn't reach their ends.
Inputs may be any that keep to these rules, and one draw needn't show every extreme that they name: `routes`: each row names two different experts; among the 12 rows of one device (aligned blocks) no expert is named more than 5 times, a bound that some block reaches.
All inputs are finite; a program needn't handle non-finite values.
Results may differ from the reference program's by a relative error of at most 0.0049.
Values may be sent and summed in bfloat16 or wider, within the bound.
A program may use at most 32 MiB of HBM per device.

```python
import math
import jax
import jax.numpy as jnp
import numpy as np
from jax import lax

D = 4096
FF = 16384
TOP = 2
TOK_DEV = 12
EXPERTS = 8
CAP = 5
TOKENS = 768


def with_spikes(entries, stream_key, source, target, shards_of, factor):
    owner, partner = [(jnp.arange(entries.shape[dim]) // (entries.shape[dim] // shards_of)).reshape([-1 if axis == dim else 1 for axis in range(entries.ndim)]) for dim in (source, target)]
    chosen = jax.random.permutation(stream_key, shards_of)[partner]
    strong = (owner == chosen) | (owner == (partner + shards_of // 2) % shards_of)
    return jnp.where(strong, factor * entries, entries)


def block_scale(key, shape, split, smallest, high):
    loudness, own = 1.0, jax.random.fold_in(key, 6)
    for dim, blocks in split:
        steps = jnp.exp(jax.random.uniform(jax.random.fold_in(own, dim), (blocks,), jnp.float32, smallest / len(split), high / len(split)))
        loudness = loudness * jnp.repeat(steps, shape[dim] // blocks).reshape([-1 if axis == dim else 1 for axis in range(len(shape))])
    return loudness


def shared_out(own_key, own, number, rows, amount, top, most, lean):
    ranking = jax.random.permutation(own_key, amount)
    crowded, usual = portions_of(amount, rows * top, most, lean, True), portions_of(amount, rows * top, most, lean, False)
    places = jnp.arange(amount)

    def named(lengths, rotation):
        used = int((lengths > 0).sum())
        fixed = max(1, used // 4)
        shifted = fixed + (places - fixed + rotation * (used - fixed)) % max(1, amount - fixed)
        return jnp.zeros((amount,), jnp.int32).at[ranking[jnp.where(places < fixed, places, shifted)]].set(jnp.asarray(lengths, jnp.int32))

    lengths = jnp.where(number % 4 == 0, named(crowded, number // 4), named(usual, number - number // 4 - 1))
    mixed = jax.random.permutation(jax.random.fold_in(own, 3), amount)
    source_of, taker = mixed[0:amount // 2 * 2:2], mixed[1:amount // 2 * 2:2]
    margin = jnp.minimum(lengths[source_of] - 1, most - lengths[taker]) // 2
    margin = jnp.where((source_of == ranking[0]) | (taker == ranking[0]) | (lengths[taker] == 0), 0, jnp.maximum(margin, 0))
    shifted = jax.random.randint(jax.random.fold_in(own, 4), (amount // 2,), 0, 1 << 20) % (margin + 1)
    lengths = lengths.at[source_of].add(-shifted).at[taker].add(shifted)
    items = jnp.searchsorted(jnp.cumsum(lengths), jnp.arange(rows * top), side="right").astype(jnp.int32)
    listing = items.reshape(top, rows).T
    listing = listing[jax.random.permutation(jax.random.fold_in(own, 1), rows)]
    rotation = jax.random.randint(jax.random.fold_in(own, 2), (rows, 1), 0, top)
    return jnp.take_along_axis(listing, (jnp.arange(top)[None, :] + rotation) % top, axis=1)


def portions_of(amount, total, most, lean, full):
    loads = [(1 << 20) // math.isqrt(grade ** lean) + 1 for grade in range(1, amount + 1)]
    largest = most if full else min(most, max(-(-total // amount), total * loads[0] // sum(loads)))
    least = 1 if total - largest >= amount - 1 else 0
    holding, surplus = [largest] + [least] * (amount - 1), total - largest - least * (amount - 1)
    while surplus > 0:
        free = [i for i in range(1, amount) if holding[i] < largest] or [i for i in range(1, amount) if holding[i] < most]
        mass, remaining = sum([loads[i] for i in free]), surplus
        for i in free:
            addition = min(most - holding[i], max(1, remaining * loads[i] // mass), surplus)
            holding[i] = holding[i] + addition
            surplus = surplus - addition
    return np.array(holding)


def bell_draw(rng, shape, width, limit, pieces=(), held_as=jnp.bfloat16):
    values = jax.random.normal(rng, shape, jnp.float32) * width
    if len(pieces) > 0:
        values = block_scale(rng, shape, pieces, -0.22, 0.18) * values
    return jnp.clip(values, min=-limit, max=limit).astype(held_as)


def noise_with(own_key, dims, spread, bound, split, heavy, kind=jnp.bfloat16):
    entries = spread * jax.random.normal(own_key, dims, jnp.float32)
    if split:
        entries = entries * block_scale(own_key, dims, split, -0.22, 0.18)
    return jnp.clip(with_spikes(entries, jax.random.fold_in(own_key, 3), *heavy), -bound, bound).astype(kind)


def setup_inputs(seed: int = 0) -> dict:
    keys = jax.random.split(jax.random.key(seed), 7)
    tokens = bell_draw(keys[0], (TOKENS, D), 1.0, 6.0, ((0, 64), (1, 16)))
    routes_keys = jax.random.split(jax.random.fold_in(keys[1], 1), TOKENS // TOK_DEV)
    routes_turns = jax.random.permutation(jax.random.fold_in(keys[1], 3), TOKENS // TOK_DEV)
    routes = jax.vmap(lambda own, number: shared_out(jax.random.fold_in(keys[1], 2), own, number, TOK_DEV, EXPERTS, TOP, CAP, 2))(routes_keys, routes_turns).reshape((TOKENS, TOP))
    router_weight = bell_draw(keys[2], (D, EXPERTS), D ** -0.5, 0.09375, ((0, 16),))
    gate_weight = bell_draw(keys[3], (EXPERTS, D, FF), D ** -0.5, 0.09375, ((0, 8), (2, 128)))
    up_weight = bell_draw(keys[4], (EXPERTS, D, FF), D ** -0.5, 0.09375, ((0, 8), (2, 128)))
    down_weight = noise_with(keys[5], (EXPERTS, FF, D), FF ** -0.5, 0.1875, ((0, 8), (1, 128)), (1, 2, 128, 5.5))
    return {"tokens": tokens, "routes": routes, "router_weight": router_weight, "gate_weight": gate_weight, "up_weight": up_weight, "down_weight": down_weight}


def reference(tokens, routes, router_weight, gate_weight, up_weight, down_weight):
    blocks = TOKENS // TOK_DEV
    logits = jnp.dot(tokens, router_weight, preferred_element_type=jnp.float32)
    labels = jnp.arange(EXPERTS, dtype=jnp.int32)
    onehot = (routes[:, :, None] == labels).astype(jnp.int32)
    chosen = jnp.sum(onehot.astype(jnp.float32) * logits[:, None, :], axis=2)
    weights = jnp.stack([jax.nn.sigmoid(chosen[:, 0] - chosen[:, 1]), jax.nn.sigmoid(chosen[:, 1] - chosen[:, 0])], axis=1)
    flat_hot = onehot.reshape(blocks, TOK_DEV * TOP, EXPERTS)
    before = jnp.cumsum(flat_hot, axis=1) - flat_hot
    position = jnp.sum(flat_hot * before, axis=2)
    places = (position[:, :, None] == jnp.arange(CAP, dtype=jnp.int32)).astype(jnp.float32)
    assign = flat_hot.astype(jnp.float32)[:, :, :, None] * places[:, :, None, :]
    assign = assign.reshape(blocks, TOK_DEV, TOP, EXPERTS, CAP)
    select = jnp.sum(assign, axis=2)
    combine = jnp.sum(assign * weights.reshape(blocks, TOK_DEV, TOP)[:, :, :, None, None], axis=2)
    grouped = tokens.reshape(blocks, TOK_DEV, D).astype(jnp.float32)
    buffers = jnp.einsum("btec,btd->ebcd", select, grouped, precision=lax.Precision.HIGHEST).astype(jnp.bfloat16)

    def expert(packed):
        inputs, w_gate, w_up, w_down = packed
        inputs = inputs.reshape(blocks * CAP, D)
        gate_part = jnp.dot(inputs, w_gate, preferred_element_type=jnp.float32)
        up_part = jnp.dot(inputs, w_up, preferred_element_type=jnp.float32)
        hidden = (jax.nn.silu(gate_part) * up_part).astype(jnp.bfloat16)
        return jnp.dot(hidden, w_down, preferred_element_type=jnp.float32).reshape(blocks, CAP, D)

    outputs = lax.map(expert, (buffers, gate_weight, up_weight, down_weight))
    mixed_out = jnp.einsum("btec,ebcd->btd", combine, outputs, precision=lax.Precision.HIGHEST)
    return mixed_out.reshape(TOKENS, D).astype(jnp.bfloat16)
```

```python
import jax
import jax.numpy as jnp
from jax import lax
from jax.experimental import pallas as pl
from jax.experimental.pallas import tpu as pltpu
from jax.sharding import PartitionSpec as P

MESH = pl.DeviceIdType.MESH
F32 = jnp.float32
BF16 = jnp.bfloat16
RING = 8
TOK = 12
CAP = 5
SLOT = 8
ROWS = 2 * RING * CAP
LANES = 128


def iota(shape, dim):
    return lax.broadcasted_iota(jnp.int32, shape, dim)


def kernel(
    tokens, routes, router, gate, up, down, out,
    tx, rx, xg, wg, wu, wd, acc, peer, hid, long_out, short_out, long_in, short_in,
    last_out, last_in, back_out, back_in, fin, logit_y, logit_z, logit_far,
    weight_local, weight_send, weight_recv, x_send, x_recv, first_send, ring_send, gather_recv,
    logit_send, logit_recv, swap_send, swap_recv, reduce_send, long_recv, short_recv,
    last_send, last_recv, back_send, back_recv,
):
    x = lax.axis_index("expert")
    dp = lax.axis_index("dp")
    mp = lax.axis_index("mp")
    core = dp % 2
    z = (mp // RING) * 4 + dp // 2
    y = mp % RING
    a1 = (1 - core) * y + core * z
    a2 = (1 - core) * z + core * y

    def device(dx, dy, dz, dcore):
        return (dx, (dz % 4) * 2 + dcore, (dz // 4) * RING + dy)

    def turned(b1, b2):
        return (1 - core) * b1 + core * b2, (1 - core) * b2 + core * b1

    def on_plane(b1, b2):
        dy, dz = turned(b1, b2)
        return device(x, dy, dz, core)

    def send(src, dst, send_sem, recv_sem, target):
        pltpu.make_async_remote_copy(
            src_ref=src, dst_ref=dst, send_sem=send_sem, recv_sem=recv_sem,
            device_id=target, device_id_type=MESH,
        ).start()

    def wait(ref, sem):
        pltpu.make_async_copy(ref, ref, sem).wait()

    barrier = pltpu.get_barrier_semaphore()

    def greet(target):
        pl.semaphore_signal(barrier, inc=1, device_id=target, device_id_type=MESH)

    for d in (4, 3, 5, 2, 6, 1, 7):
        greet(device((x + d) % RING, y, z, core))
        greet(device((x + d) % RING, y, z, 1 - core))
        greet(device(x, (y + d) % RING, z, core))
        greet(device(x, y, (z + d) % RING, core))
    greet(device(x, y, z, 1 - core))

    pltpu.make_async_copy(
        gate.at[:, core], wg.at[:, :, pl.ds(pl.multiple_of(core * LANES, LANES), LANES)], weight_local.at[0]
    ).start()
    pltpu.make_async_copy(
        up.at[:, core], wu.at[:, :, pl.ds(pl.multiple_of(core * LANES, LANES), LANES)], weight_local.at[1]
    ).start()

    def down_columns(block, half):
        return down.at[:, pl.ds(pl.multiple_of((block * 2 + half) * LANES, LANES), LANES)]

    def down_rows(block):
        return wd.at[block, pl.ds(pl.multiple_of(core * LANES, LANES), LANES)]

    @pl.loop(0, 2 * RING)
    def _(block):
        pltpu.make_async_copy(down_columns(block, core), down_rows(block), weight_local.at[2]).start()

    r0 = routes[:, 0:1]
    r1 = routes[:, 1:2]
    lane = iota((TOK, LANES), 1)
    hot0 = r0 == lane // SLOT
    hot1 = r1 == lane // SLOT
    hot = jnp.where(hot0 | hot1, 1.0, 0.0)
    earlier = jnp.where(iota((TOK, TOK), 1) < iota((TOK, TOK), 0), 1.0, 0.0)
    before = jnp.dot(earlier.astype(BF16), hot.astype(BF16), preferred_element_type=F32)
    assign = jnp.where(before == (lane % SLOT).astype(F32), hot, 0.0)
    tok = tokens[...]
    chosen = lax.dot_general(
        assign.astype(BF16), tok, (((0,), (0,)), ((), ())), preferred_element_type=F32
    )
    for e in range(RING):
        for half in range(2):
            tx[e * 2 + half] = chosen[
                e * SLOT : (e + 1) * SLOT, half * LANES : (half + 1) * LANES
            ].astype(BF16)

    spread = jnp.where(iota((RING, LANES), 1) % RING == iota((RING, LANES), 0), 1.0, 0.0)
    router_wide = jnp.dot(router[...], spread.astype(BF16), preferred_element_type=F32).astype(BF16)
    term = jnp.dot(tok, router_wide, preferred_element_type=F32)
    own_lanes = lane // RING == iota((TOK, LANES), 0)
    logit_y[0] = jnp.sum(jnp.where(own_lanes, term, 0.0), axis=0, keepdims=True)
    acc[...] = jnp.zeros_like(acc)
    me_x = x * 2 + core
    rx[me_x] = tx[me_x]

    pl.semaphore_wait(barrier, 4 * (RING - 1) + 1)

    for d in (4, 3, 5, 2, 6, 1, 7, 0):
        e = (x + d) % RING
        send(tx.at[e * 2 + 1 - core], rx.at[me_x], x_send, x_recv, device(e, y, z, 1 - core))
        if d:
            send(tx.at[e * 2 + core], rx.at[me_x], x_send, x_recv, device(e, y, z, core))
    for d in (4, 3, 5, 2, 6, 1, 7):
        send(logit_y.at[0], logit_y.at[d], logit_send.at[0], logit_recv.at[0], device(x, (y + d) % RING, z, core))

    partner = device(x, y, z, 1 - core)
    send(
        gate.at[:, 1 - core], wg.at[:, :, pl.ds(pl.multiple_of(core * LANES, LANES), LANES)],
        weight_send.at[0], weight_recv.at[0], partner,
    )
    send(
        up.at[:, 1 - core], wu.at[:, :, pl.ds(pl.multiple_of(core * LANES, LANES), LANES)],
        weight_send.at[1], weight_recv.at[1], partner,
    )

    @pl.loop(0, 2 * RING)
    def _(block):
        send(down_columns(block, 1 - core), down_rows(block), weight_send.at[2], weight_recv.at[2], partner)

    wait(rx.at[pl.ds(0, 15)], x_recv)
    packed = jnp.where(
        iota((ROWS, LANES), 1) == (iota((ROWS, LANES), 0) // CAP) * SLOT + iota((ROWS, LANES), 0) % CAP, 1.0, 0.0
    ).astype(BF16)
    arrived = rx[...].astype(F32).reshape(2 * RING * SLOT, LANES).astype(BF16)
    xg[0, 0] = jnp.dot(packed, arrived, preferred_element_type=F32).astype(BF16)
    for d in (4, 3, 5, 2, 6, 1, 7):
        send(xg.at[0, 0], xg.at[0, d], first_send, gather_recv.at[0, d], on_plane((a1 + d) % RING, a2))

    def forward(d2, d1, to):
        step = 1 if to < 5 and to > d2 else RING - 1
        send(xg.at[d2, d1], xg.at[to, d1], ring_send, gather_recv.at[to, d1], on_plane(a1, (a2 + step) % RING))

    def multiply(d2, d1):
        oy, oz = turned((a1 + RING - d1) % RING, (a2 + RING - d2) % RING)
        group = oz % 4
        block = (oz // 4) * RING + oy
        piece = xg[d2, d1]
        return group, jnp.dot(piece, wg[block], preferred_element_type=F32), jnp.dot(
            piece, wu[block], preferred_element_type=F32
        )

    def gather_event(level, d1, first=False):
        if level == 0:
            if not first:
                wait(xg.at[0, d1], gather_recv.at[0, d1])
            forward(0, d1, 1)
            forward(0, d1, 7)
            sides = (0,)
        elif level < 4:
            sides = (level, RING - level)
            for side in sides:
                wait(xg.at[side, d1], gather_recv.at[side, d1])
                if level < 3:
                    forward(side, d1, side + 1 if side < 4 else side - 1)
                else:

                    @pl.when(d1 % 2 == (0 if side < 4 else 1))
                    def _(side=side):
                        send(
                            xg.at[side, d1], xg.at[4, d1], ring_send, gather_recv.at[4, d1],
                            on_plane(a1, (a2 + (1 if side < 4 else RING - 1)) % RING),
                        )
        else:
            sides = (4,)
            wait(xg.at[4, d1], gather_recv.at[4, d1])
        products = [multiply(side, d1) for side in sides]
        for group, by_gate, by_up in products:
            acc[group, 0] += by_gate
            acc[group, 1] += by_up

    def outward(k):
        return (k % 2) * ((k + 1) // 2) + (1 - k % 2) * ((RING - k // 2) % RING)

    def weights_there():
        wait(gate.at[:, core], weight_local.at[0])
        wait(up.at[:, core], weight_local.at[1])
        wait(gate.at[:, core], weight_recv.at[0])
        wait(up.at[:, core], weight_recv.at[1])

    forward(0, 0, 1)
    forward(0, 0, 7)
    weights_there()
    group, by_gate, by_up = multiply(0, 0)
    acc[group, 0] += by_gate
    acc[group, 1] += by_up
    for wave in range(5):
        if wave < 4:
            gather_event(wave + 1, 0)

        @pl.loop(1, RING)
        def _(k, wave=wave):
            gather_event(wave, outward(k))

    for g in range(4):
        send(acc.at[g], peer.at[g], swap_send, swap_recv.at[g], partner)

    wait(logit_y.at[pl.ds(0, 7)], logit_recv.at[0])
    logit_z[...] = jnp.sum(logit_y[...], axis=0)
    send(logit_z, logit_far, logit_send.at[1], logit_recv.at[1], device(x, y, (z + 4) % RING, core))

    for g in range(4):
        wait(peer.at[g], swap_recv.at[g])
        by_gate = acc[g, 0] + peer[g, 0]
        by_up = acc[g, 1] + peer[g, 1]
        hid[g] = (by_gate / (1.0 + jnp.exp(-by_gate)) * by_up).astype(BF16)

    wait(wd.at[pl.ds(0, 8)], weight_local.at[2])
    wait(wd.at[pl.ds(0, 8)], weight_recv.at[2])

    def partial(d2, d1):
        ty, tz = turned((a1 + d1) % RING, (a2 + d2 + RING) % RING)
        return jnp.dot(hid[tz % 4], wd[(tz // 4) * RING + ty], preferred_element_type=F32)

    for turn in range(4):

        @pl.loop(0, RING)
        def _(k, turn=turn):
            d1 = outward(RING - 1 - k)
            sign = 1 - 2 * (d1 % 2)
            far = partial(sign * (4 - turn), d1)
            near = partial(-sign * (3 - turn), d1) if turn < 3 else None
            if turn:
                wait(long_in.at[turn - 1, d1], long_recv.at[turn - 1, d1])
                far += long_in[turn - 1, d1].astype(F32)
            long_out[turn, d1] = far.astype(BF16)
            send(
                long_out.at[turn, d1], long_in.at[turn, d1], reduce_send.at[0], long_recv.at[turn, d1],
                on_plane(a1, (a2 + sign + RING) % RING),
            )
            if turn < 3:
                if turn:
                    wait(short_in.at[turn - 1, d1], short_recv.at[turn - 1, d1])
                    near += short_in[turn - 1, d1].astype(F32)
                short_out[turn, d1] = near.astype(BF16)
                send(
                    short_out.at[turn, d1], short_in.at[turn, d1], reduce_send.at[1], short_recv.at[turn, d1],
                    on_plane(a1, (a2 - sign + RING) % RING),
                )

    def reduced(d1):
        own = partial(0, d1)
        wait(long_in.at[3, d1], long_recv.at[3, d1])
        wait(short_in.at[2, d1], short_recv.at[2, d1])
        return own + long_in[3, d1].astype(F32) + short_in[2, d1].astype(F32)

    @pl.loop(0, RING - 1)
    def _(k):
        d1 = outward(RING - 1 - k)
        last_out[d1] = reduced(d1).astype(BF16)
        send(last_out.at[d1], last_in.at[d1], last_send, last_recv.at[d1], on_plane((a1 + d1) % RING, a2))

    fin[...] = reduced(0)

    wait(logit_far, logit_recv.at[1])
    logits = logit_z[...] + logit_far[...]
    signs = jnp.where(lane % RING == r0, 1.0, 0.0) - jnp.where(lane % RING == r1, 1.0, 0.0)
    gap = jnp.sum(jnp.where(own_lanes, signs * logits, 0.0), axis=1, keepdims=True)
    weight = jnp.where(hot0, 1.0 / (1.0 + jnp.exp(-gap)), 1.0 / (1.0 + jnp.exp(gap)))
    combine = (assign * weight)[:, : RING * SLOT]

    total = fin[...]
    for d in (1, 7, 2, 6, 3, 5, 4):
        wait(last_in.at[d], last_recv.at[d])
        total += last_in[d].astype(F32)

    unpacked = jnp.where(
        iota((LANES, ROWS), 0) == (iota((LANES, ROWS), 1) // CAP) * SLOT + iota((LANES, ROWS), 1) % CAP, 1.0, 0.0
    ).astype(BF16)
    opened = jnp.dot(unpacked, total.astype(BF16), preferred_element_type=F32)
    for i in range(2 * RING):
        back_out[i] = opened[i * SLOT : (i + 1) * SLOT].astype(BF16)
    for d in (4, 3, 5, 2, 6, 1, 7, 0):
        i = (x + d) % RING
        send(back_out.at[i * 2 + 1 - core], back_in.at[core, x], back_send, back_recv, device(i, y, z, 1 - core))
        if d:
            send(back_out.at[i * 2 + core], back_in.at[core, x], back_send, back_recv, device(i, y, z, core))
    back_in[core, x] = back_out[me_x]

    wait(tx.at[pl.ds(0, 15)], x_send)
    wait(logit_y.at[pl.ds(0, 7)], logit_send.at[0])
    wait(logit_z, logit_send.at[1])
    wait(gate.at[:, core], weight_send.at[0])
    wait(up.at[:, core], weight_send.at[1])
    wait(wd.at[pl.ds(0, 8)], weight_send.at[2])
    wait(xg.at[0, pl.ds(0, 7)], first_send)
    wait(xg.at[pl.ds(0, 7)], ring_send)
    wait(acc, swap_send)
    wait(long_out, reduce_send.at[0])
    wait(short_out, reduce_send.at[1])
    wait(last_out.at[pl.ds(0, 7)], last_send)

    wait(back_out.at[pl.ds(0, 15)], back_recv)
    for half in range(2):
        pieces = back_in[half].astype(F32).reshape(RING * SLOT, LANES)
        out[:, half * LANES : (half + 1) * LANES] = jnp.dot(
            combine, pieces, precision=lax.Precision.HIGHEST, preferred_element_type=F32
        ).astype(BF16)
    wait(back_out.at[pl.ds(0, 15)], back_send)


def per_device(tokens, routes, router_weight, gate_weight, up_weight, down_weight):
    blocks, width = 2 * RING, 2 * LANES
    dma = pltpu.SemaphoreType.DMA
    vmem = pltpu.VMEM
    in_vmem = pl.BlockSpec(memory_space=pltpu.VMEM)
    in_hbm = pl.BlockSpec(memory_space=pl.ANY)
    return pl.pallas_call(
        kernel,
        out_shape=jax.ShapeDtypeStruct((TOK, width), BF16),
        in_specs=[in_vmem] * 3 + [in_hbm] * 3,
        out_specs=in_vmem,
        scratch_shapes=[
            vmem((blocks, SLOT, LANES), BF16),
            vmem((blocks, SLOT, LANES), BF16),
            vmem((RING, RING, ROWS, LANES), BF16),
            vmem((blocks, LANES, width), BF16),
            vmem((blocks, LANES, width), BF16),
            vmem((blocks, width, LANES), BF16),
            vmem((4, 2, ROWS, width), F32),
            vmem((4, 2, ROWS, width), F32),
            vmem((4, ROWS, width), BF16),
            vmem((4, RING, ROWS, LANES), BF16),
            vmem((3, RING, ROWS, LANES), BF16),
            vmem((4, RING, ROWS, LANES), BF16),
            vmem((3, RING, ROWS, LANES), BF16),
            vmem((RING, ROWS, LANES), BF16),
            vmem((RING, ROWS, LANES), BF16),
            vmem((blocks, SLOT, LANES), BF16),
            vmem((2, RING, SLOT, LANES), BF16),
            vmem((ROWS, LANES), F32),
            vmem((RING, 1, LANES), F32),
            vmem((1, LANES), F32),
            vmem((1, LANES), F32),
            dma((3,)),
            dma((3,)),
            dma((3,)),
            dma,
            dma,
            dma,
            dma,
            dma((RING, RING)),
            dma((2,)),
            dma((2,)),
            dma,
            dma((4,)),
            dma((2,)),
            dma((4, RING)),
            dma((3, RING)),
            dma,
            dma((RING,)),
            dma,
            dma,
        ],
        compiler_params=pltpu.CompilerParams(collective_id=0, has_side_effects=True),
        name="moe",
    )(
        tokens,
        routes,
        router_weight,
        gate_weight.reshape(blocks, 2, LANES, LANES),
        up_weight.reshape(blocks, 2, LANES, LANES),
        down_weight[0],
    )


def solution(mesh):
    return jax.shard_map(
        per_device,
        mesh=mesh,
        in_specs=(
            P(("expert", "dp"), "mp"),
            P(("expert", "dp"), None),
            P("mp", None),
            P("expert", None, ("dp", "mp")),
            P("expert", None, ("dp", "mp")),
            P("expert", ("dp", "mp"), None),
        ),
        out_specs=P(("expert", "dp"), "mp"),
        check_vma=False,
    )
```

```python
import jax
import jax.numpy as jnp
from jax import lax
from jax.experimental import pallas as pl
from jax.experimental.pallas import tpu as pltpu
from jax.sharding import PartitionSpec as P

MESH = pl.DeviceIdType.MESH
F32 = jnp.float32
BF16 = jnp.bfloat16
RING = 8
TOK = 12
CAP = 5
SLOT = 8
ROWS = 2 * RING * CAP
LANES = 128


def iota(shape, dim):
    return lax.broadcasted_iota(jnp.int32, shape, dim)


def kernel(
    tokens, routes, router, gate, up, down, out,
    tx, rx, xg, wg, wu, wd_z, wd_y, acc, peer, hid, part, reduce_out, reduce_in,
    last_out, last_in, back_out, back_in, fin, router_here, logit_y, logit_z, logit_far,
    weight_local, weight_send, weight_recv, x_send, x_recv, first_send, first_recv, ring_send, pair_recv, batch_recv,
    logit_send, logit_recv, swap_send, swap_recv, reduce_send, reduce_recv,
    last_send, last_recv, back_send, back_recv,
):
    x = lax.axis_index("expert")
    dp = lax.axis_index("dp")
    mp = lax.axis_index("mp")
    core = dp % 2
    z = (mp // RING) * 4 + dp // 2
    y = mp % RING
    a1 = (1 - core) * y + core * z
    a2 = (1 - core) * z + core * y

    def device(dx, dy, dz, dcore):
        return (dx, (dz % 4) * 2 + dcore, (dz // 4) * RING + dy)

    def on_plane(b1, b2):
        return device(x, (1 - core) * b1 + core * b2, (1 - core) * b2 + core * b1, core)

    def send(src, dst, send_sem, recv_sem, target):
        pltpu.make_async_remote_copy(
            src_ref=src, dst_ref=dst, send_sem=send_sem, recv_sem=recv_sem,
            device_id=target, device_id_type=MESH,
        ).start()

    def wait(ref, sem):
        pltpu.make_async_copy(ref, ref, sem).wait()

    def outward(k):
        return (k % 2) * ((k + 1) // 2) + (1 - k % 2) * ((RING - k // 2) % RING)

    def near_first(k):
        return (a1 + outward(k)) % RING

    def far_first(k):
        return (a1 + outward(RING - 1 - k)) % RING

    barrier = pltpu.get_barrier_semaphore()

    def greet(target):
        pl.semaphore_signal(barrier, inc=1, device_id=target, device_id_type=MESH)

    for d in (4, 3, 5, 2, 6, 1, 7):
        greet(device((x + d) % RING, y, z, core))
        greet(device((x + d) % RING, y, z, 1 - core))
        greet(device(x, (y + d) % RING, z, core))
        greet(device(x, y, (z + d) % RING, core))
    greet(device(x, y, z, 1 - core))

    pltpu.make_async_copy(router, router_here, weight_local.at[3]).start()

    r0 = routes[0:1, :]
    r1 = routes[1:2, :]
    row = iota((RING * SLOT, TOK), 0)
    hot0 = r0 == row // SLOT
    hot = jnp.where(hot0 | (r1 == row // SLOT), 1.0, 0.0)
    earlier = jnp.where(iota((TOK, TOK), 0) < iota((TOK, TOK), 1), 1.0, 0.0)
    before = jnp.dot(hot.astype(BF16), earlier.astype(BF16), preferred_element_type=F32)
    assign = jnp.where(before == (row % SLOT).astype(F32), hot, 0.0)
    tok = tokens[...]
    chosen = jnp.dot(assign.astype(BF16), tok, preferred_element_type=F32)
    for e in range(RING):
        for half in range(2):
            tx[e * 2 + half] = chosen[
                e * SLOT : (e + 1) * SLOT, half * LANES : (half + 1) * LANES
            ].astype(BF16)
    me_x = x * 2 + core
    rx[me_x] = tx[me_x]

    pl.semaphore_wait(barrier, 4 * (RING - 1) + 1)

    for d in (4, 3, 5, 2, 6, 1, 7, 0):
        e = (x + d) % RING
        send(tx.at[e * 2 + 1 - core], rx.at[me_x], x_send, x_recv, device(e, y, z, 1 - core))
        if d:
            send(tx.at[e * 2 + core], rx.at[me_x], x_send, x_recv, device(e, y, z, core))

    partner = device(x, y, z, 1 - core)
    units = pl.ds(pl.multiple_of(core * LANES, LANES), LANES)

    def down_columns(block, half):
        return down.at[:, pl.ds(pl.multiple_of((block * 2 + half) * LANES, LANES), LANES)]

    @pl.loop(0, 2 * RING)
    def _(block):
        high, wy = block // RING, block % RING
        for half in range(2):
            place = block if half == 0 else wy * 2 + high
            if half == 0:
                down_place = wd_z.at[high, units, pl.ds(pl.multiple_of(wy * LANES, LANES), LANES)]
            else:
                down_place = wd_y.at[wy, units, pl.ds(pl.multiple_of(high * LANES, LANES), LANES)]
            moves = (
                (gate.at[block, half], wg.at[place, :, units]),
                (up.at[block, half], wu.at[place, :, units]),
                (down_columns(block, half), down_place),
            )

            @pl.when(core == half)
            def _(moves=moves):
                for i, (src, dst) in enumerate(moves):
                    pltpu.make_async_copy(src, dst, weight_local.at[i]).start()

            @pl.when(core != half)
            def _(moves=moves):
                for i, (src, dst) in enumerate(moves):
                    send(src, dst, weight_send.at[i], weight_recv.at[i], partner)

    own_lanes = iota((RING, LANES), 1) % RING == iota((RING, LANES), 0)
    of_token = jnp.where(iota((TOK, LANES), 1) // RING == iota((TOK, LANES), 0), 1.0, 0.0)
    wait(router_here, weight_local.at[3])
    term = lax.dot_general(router_here[...], tok, (((1,), (1,)), ((), ())), preferred_element_type=F32)
    wide = jnp.dot(term, of_token, precision=lax.Precision.HIGHEST, preferred_element_type=F32)
    logit_y[0] = jnp.sum(jnp.where(own_lanes, wide, 0.0), axis=0, keepdims=True)
    for d in (4, 3, 5, 2, 6, 1, 7):
        send(logit_y.at[0], logit_y.at[d], logit_send.at[0], logit_recv.at[0], device(x, (y + d) % RING, z, core))
    acc[...] = jnp.zeros_like(acc)
    packed = jnp.where(
        iota((ROWS, LANES), 1) == (iota((ROWS, LANES), 0) // CAP) * SLOT + iota((ROWS, LANES), 0) % CAP, 1.0, 0.0
    ).astype(BF16)

    wait(rx.at[pl.ds(0, 15)], x_recv)
    arrived = rx[...].astype(F32).reshape(2 * RING * SLOT, LANES).astype(BF16)
    xg[0, a1] = jnp.dot(packed, arrived, preferred_element_type=F32).astype(BF16)
    for d in (1, 7, 2, 6, 3, 5, 4):
        send(xg.at[0, a1], xg.at[0, a1], first_send, first_recv.at[a1], on_plane((a1 + d) % RING, a2))

    def along(d2, j, to, hop, sem):
        send(xg.at[d2, j], xg.at[to, j], ring_send, sem, on_plane(a1, (a2 + hop + RING) % RING))

    def to_second(j):
        along(0, j, 2, 2, pair_recv.at[j])
        along(0, j, 6, -2, pair_recv.at[j])

    def to_next(j):
        along(0, j, 1, 1, batch_recv.at[1])
        along(0, j, 7, -1, batch_recv.at[7])

    def from_second(j):
        wait(xg.at[pl.ds(0, 2), j], pair_recv.at[j])
        for i, (at, sign) in enumerate(((2, 1), (6, -1))):

            @pl.when(j % 2 == i)
            def _(at=at, sign=sign):
                along(at, j, 4, 2 * sign, batch_recv.at[4])

            along(at, j, at + sign, sign, batch_recv.at[at + sign])

    def multiply(d2):
        origin = (a2 + RING - d2) % RING

        @pl.when(core == 0)
        def _():
            rows = jnp.concatenate([xg[d2, j] for j in range(RING)], axis=1)
            group, first = origin % 4, (origin // 4) * RING
            for i, w in enumerate((wg, wu)):
                acc[group, i] += jnp.dot(
                    rows, w[pl.ds(first, RING)].reshape(RING * LANES, 2 * LANES), preferred_element_type=F32
                )

        @pl.when(core == 1)
        def _():
            rows = jnp.concatenate(
                [xg[d2, 0:4].reshape(4 * ROWS, LANES), xg[d2, 4:8].reshape(4 * ROWS, LANES)], axis=1
            )
            for i, w in enumerate((wg, wu)):
                acc[:, i] += jnp.dot(
                    rows, w[pl.ds(origin * 2, 2)].reshape(2 * LANES, 2 * LANES), preferred_element_type=F32
                ).reshape(4, ROWS, 2 * LANES)

    def first_event(k):
        j = near_first(k)
        wait(xg.at[0, j], first_recv.at[j])
        to_second(j)

    to_second(a1)
    to_next(a1)
    first_event(1)
    first_event(2)
    from_second(a1)

    @pl.loop(3, RING)
    def _(k):
        first_event(k)

    for i in range(2):
        wait(wg.at[pl.ds(0, 8)], (weight_local, weight_recv)[i].at[0])
        wait(wu.at[pl.ds(0, 8)], (weight_local, weight_recv)[i].at[1])
    multiply(0)

    @pl.loop(1, 5)
    def _(k):
        to_next(near_first(k))

    @pl.loop(1, RING)
    def _(k):
        from_second(near_first(k))

        @pl.when(k > 4)
        def _():
            to_next(near_first(k))

    def swap(g):
        send(acc.at[g], peer.at[g], swap_send, swap_recv.at[g], partner)

    def swap_done(d2):
        @pl.when(core == 0)
        def _():
            swap((a2 + RING - d2) % 4)

    multiply(2)
    multiply(6)
    swap_done(2)
    for d2 in (1, 7, 3, 5, 4):
        wait(xg.at[d2], batch_recv.at[d2])
        multiply(d2)
        if d2 in (3, 5, 4):
            swap_done(d2)

    @pl.when(core == 1)
    def _():
        for g in range(4):
            swap(g)

    wait(logit_y.at[pl.ds(0, 7)], logit_recv.at[0])
    logit_z[...] = jnp.sum(logit_y[...], axis=0)
    send(logit_z, logit_far, logit_send.at[1], logit_recv.at[1], device(x, y, (z + 4) % RING, core))
    for i in range(2):
        wait(wd_z.at[0], (weight_local, weight_recv)[i].at[2])

    for g in range(4):
        wait(peer.at[g], swap_recv.at[g])
        by_gate = acc[g, 0] + peer[g, 0]
        by_up = acc[g, 1] + peer[g, 1]
        hid[g] = (by_gate / (1.0 + jnp.exp(-by_gate)) * by_up).astype(BF16)

    def partial(d2, put):
        target = (a2 + d2 + RING) % RING

        @pl.when(core == 0)
        def _():
            terms = jnp.dot(hid[target % 4], wd_z[target // 4], preferred_element_type=F32)
            for j in range(RING):
                put(j, terms[:, j * LANES : (j + 1) * LANES])

        @pl.when(core == 1)
        def _():
            terms = jnp.dot(hid[...].reshape(4 * ROWS, 2 * LANES), wd_y[target], preferred_element_type=F32)
            for j in range(RING):
                low, high = j % 4, j // 4
                put(j, terms[low * ROWS : (low + 1) * ROWS, high * LANES : (high + 1) * LANES])

    def hop_on(m, j, hop):
        send(
            reduce_out.at[m, j], reduce_in.at[m, j], reduce_send, reduce_recv.at[m // 3 - m // 6, j],
            on_plane(a1, (a2 + hop + RING) % RING),
        )

    def put_out(m):
        def put(j, value):
            reduce_out[m, j] = value.astype(BF16)

        return put

    def put_part(i):
        def put(j, value):
            part[i, j] = value

        return put

    partial(4, put_out(0))

    @pl.loop(0, RING)
    def _(k):
        j = far_first(k)
        hop_on(0, j, 2 - 4 * (j % 2))

    for m, d2, hop in ((1, 3, 1), (2, -3, -1), (3, 1, 1), (4, -1, -1)):
        partial(d2, put_out(m))

        @pl.loop(0, RING)
        def _(k, m=m, hop=hop):
            hop_on(m, far_first(k), hop)

    partial(2, put_part(0))
    partial(-2, put_part(1))

    @pl.loop(0, RING)
    def _(k):
        j = far_first(k)
        wait(reduce_in.at[pl.ds(0, 3), j], reduce_recv.at[0, j])
        fourth = reduce_in[0, j].astype(F32)
        even = j % 2 == 0
        ahead = part[0, j] + reduce_in[1, j].astype(F32) + jnp.where(even, fourth, 0.0)
        behind = part[1, j] + reduce_in[2, j].astype(F32) + jnp.where(even, 0.0, fourth)
        reduce_out[5, j] = ahead.astype(BF16)
        hop_on(5, j, 2)
        reduce_out[6, j] = behind.astype(BF16)
        hop_on(6, j, -2)

    partial(0, put_part(2))

    def reduced(j):
        total = part[2, j]
        wait(reduce_in.at[pl.ds(3, 4), j], reduce_recv.at[1, j])
        for m in range(3, 7):
            total += reduce_in[m, j].astype(F32)
        return total

    @pl.loop(0, RING - 1)
    def _(k):
        j = far_first(k)
        last_out[j] = reduced(j).astype(BF16)
        send(last_out.at[j], last_in.at[a1], last_send, last_recv, on_plane(j, a2))

    fin[...] = reduced(a1)

    wait(logit_far, logit_recv.at[1])
    logits = jnp.where(own_lanes, logit_z[...] + logit_far[...], 0.0)
    logits = lax.dot_general(
        logits, of_token, (((1,), (1,)), ((), ())), precision=lax.Precision.HIGHEST, preferred_element_type=F32
    )
    expert = iota((RING, TOK), 0)
    gap = jnp.sum(jnp.where(r0 == expert, logits, 0.0) - jnp.where(r1 == expert, logits, 0.0), axis=0, keepdims=True)
    combine = assign * jnp.where(hot0, 1.0 / (1.0 + jnp.exp(-gap)), 1.0 / (1.0 + jnp.exp(gap)))
    unpacked = jnp.where(
        iota((LANES, ROWS), 0) == (iota((LANES, ROWS), 1) // CAP) * SLOT + iota((LANES, ROWS), 1) % CAP, 1.0, 0.0
    ).astype(BF16)

    total = fin[...]
    wait(last_in.at[pl.ds(0, 7)], last_recv)
    for d in range(1, RING):
        total += last_in[(a1 + d) % RING].astype(F32)

    opened = jnp.dot(unpacked, total.astype(BF16), preferred_element_type=F32)
    for i in range(2 * RING):
        back_out[i] = opened[i * SLOT : (i + 1) * SLOT].astype(BF16)
    for d in (4, 3, 5, 2, 6, 1, 7, 0):
        i = (x + d) % RING
        send(back_out.at[i * 2 + 1 - core], back_in.at[core, x], back_send, back_recv, device(i, y, z, 1 - core))
        if d:
            send(back_out.at[i * 2 + core], back_in.at[core, x], back_send, back_recv, device(i, y, z, core))
    back_in[core, x] = back_out[me_x]

    wait(tx.at[pl.ds(0, 15)], x_send)
    wait(logit_y.at[pl.ds(0, 7)], logit_send.at[0])
    wait(logit_z, logit_send.at[1])
    wait(wg.at[pl.ds(0, 8)], weight_send.at[0])
    wait(wu.at[pl.ds(0, 8)], weight_send.at[1])
    wait(wd_z.at[0], weight_send.at[2])
    wait(xg.at[0, pl.ds(0, 7)], first_send)
    wait(xg.at[pl.ds(0, 7)], ring_send)
    wait(acc, swap_send)
    wait(reduce_out, reduce_send)
    wait(last_out.at[pl.ds(0, 7)], last_send)

    wait(back_out.at[pl.ds(0, 15)], back_recv)
    for half in range(2):
        pieces = back_in[half].astype(F32).reshape(RING * SLOT, LANES)
        out[:, half * LANES : (half + 1) * LANES] = lax.dot_general(
            combine, pieces, (((0,), (0,)), ((), ())), precision=lax.Precision.HIGHEST, preferred_element_type=F32
        ).astype(BF16)
    wait(back_out.at[pl.ds(0, 15)], back_send)


def per_device(tokens, routes, router_weight, gate_weight, up_weight, down_weight):
    blocks, width = 2 * RING, 2 * LANES
    dma = pltpu.SemaphoreType.DMA
    vmem = pltpu.VMEM
    in_vmem = pl.BlockSpec(memory_space=pltpu.VMEM)
    in_hbm = pl.BlockSpec(memory_space=pltpu.HBM)
    return pl.pallas_call(
        kernel,
        out_shape=jax.ShapeDtypeStruct((TOK, width), BF16),
        in_specs=[in_vmem] * 2 + [in_hbm] * 4,
        out_specs=in_vmem,
        scratch_shapes=[
            vmem((blocks, SLOT, LANES), BF16),
            vmem((blocks, SLOT, LANES), BF16),
            vmem((RING, RING, ROWS, LANES), BF16),
            vmem((blocks, LANES, width), BF16),
            vmem((blocks, LANES, width), BF16),
            vmem((2, width, RING * LANES), BF16),
            vmem((RING, width, width), BF16),
            vmem((4, 2, ROWS, width), F32),
            vmem((4, 2, ROWS, width), F32),
            vmem((4, ROWS, width), BF16),
            vmem((3, RING, ROWS, LANES), F32),
            vmem((7, RING, ROWS, LANES), BF16),
            vmem((7, RING, ROWS, LANES), BF16),
            vmem((RING, ROWS, LANES), BF16),
            vmem((RING, ROWS, LANES), BF16),
            vmem((blocks, SLOT, LANES), BF16),
            vmem((2, RING, SLOT, LANES), BF16),
            vmem((ROWS, LANES), F32),
            vmem((RING, width), BF16),
            vmem((RING, 1, LANES), F32),
            vmem((1, LANES), F32),
            vmem((1, LANES), F32),
            dma((4,)),
            dma((3,)),
            dma((3,)),
            dma,
            dma,
            dma,
            dma((RING,)),
            dma,
            dma((RING,)),
            dma((RING,)),
            dma((2,)),
            dma((2,)),
            dma,
            dma((4,)),
            dma,
            dma((2, RING)),
            dma,
            dma,
            dma,
            dma,
        ],
        compiler_params=pltpu.CompilerParams(collective_id=0, has_side_effects=True, vmem_limit_bytes=40 * 2**20),
        name="moe",
    )(
        tokens,
        routes.T,
        *(
            pltpu.with_memory_space_constraint(w, pltpu.HBM)
            for w in (
                router_weight.T,
                gate_weight.reshape(blocks, 2, LANES, LANES),
                up_weight.reshape(blocks, 2, LANES, LANES),
                down_weight[0],
            )
        ),
    )


def solution(mesh):
    return jax.shard_map(
        per_device,
        mesh=mesh,
        in_specs=(
            P(("expert", "dp"), "mp"),
            P(("expert", "dp"), None),
            P("mp", None),
            P("expert", None, ("dp", "mp")),
            P("expert", None, ("dp", "mp")),
            P("expert", ("dp", "mp"), None),
        ),
        out_specs=P(("expert", "dp"), "mp"),
        check_vma=False,
    )
```

```python
import jax
import jax.numpy as jnp
from jax import lax
from jax.experimental import pallas as pl
from jax.experimental.pallas import tpu as pltpu
from jax.sharding import PartitionSpec as P

MESH = pl.DeviceIdType.MESH
F32 = jnp.float32
BF16 = jnp.bfloat16
RING = 8
TOK = 12
CAP = 5
SLOT = 8
ROWS = 2 * RING * CAP
LANES = 128


def iota(shape, dim):
    return lax.broadcasted_iota(jnp.int32, shape, dim)


def kernel(
    tokens, routes, router, gate, up, down, out,
    tx, rx, xg, wg, wu, wd_z, wd_y, acc, peer, hid, part, reduce_out, reduce_in,
    last_out, last_in, back_out, back_in, fin, tokens_here, routes_here, router_here, logit_y, logit_z, logit_far,
    weight_local, weight_send, weight_recv, x_send, x_recv, first_send, first_recv, ring_send, pair_recv, batch_recv,
    logit_send, logit_recv, swap_send, swap_recv, reduce_send, reduce_recv,
    last_send, last_recv, back_send, back_recv,
):
    x = lax.axis_index("expert")
    dp = lax.axis_index("dp")
    mp = lax.axis_index("mp")
    core = dp % 2
    z = (mp // RING) * 4 + dp // 2
    y = mp % RING
    a1 = (1 - core) * y + core * z
    a2 = (1 - core) * z + core * y

    def device(dx, dy, dz, dcore):
        return (dx, (dz % 4) * 2 + dcore, (dz // 4) * RING + dy)

    def on_plane(b1, b2):
        return device(x, (1 - core) * b1 + core * b2, (1 - core) * b2 + core * b1, core)

    def send(src, dst, send_sem, recv_sem, target):
        pltpu.make_async_remote_copy(
            src_ref=src, dst_ref=dst, send_sem=send_sem, recv_sem=recv_sem,
            device_id=target, device_id_type=MESH,
        ).start()

    def wait(ref, sem):
        pltpu.make_async_copy(ref, ref, sem).wait()

    def outward(k):
        return (k % 2) * ((k + 1) // 2) + (1 - k % 2) * ((RING - k // 2) % RING)

    def near_first(k):
        return (a1 + outward(k)) % RING

    def far_first(k):
        return (a1 + outward(RING - 1 - k)) % RING

    small = ((routes, routes_here), (tokens, tokens_here), (router, router_here))
    small = [pltpu.make_async_copy(*pair, weight_local.at[3 + i]) for i, pair in enumerate(small)]
    for copy in small:
        copy.start()
    barrier = pltpu.get_barrier_semaphore()

    def greet(target):
        pl.semaphore_signal(barrier, inc=1, device_id=target, device_id_type=MESH)

    for d in (4, 3, 5, 2, 6, 1, 7):
        greet(device((x + d) % RING, y, z, core))
        greet(device((x + d) % RING, y, z, 1 - core))
        greet(device(x, (y + d) % RING, z, core))
        greet(device(x, y, (z + d) % RING, core))
    greet(device(x, y, z, 1 - core))

    small[0].wait()
    r0 = routes_here[0:1, :]
    r1 = routes_here[1:2, :]
    row = iota((RING * SLOT, TOK), 0)
    hot0 = r0 == row // SLOT
    hot = jnp.where(hot0 | (r1 == row // SLOT), 1.0, 0.0)
    earlier = jnp.where(iota((TOK, TOK), 0) < iota((TOK, TOK), 1), 1.0, 0.0)
    before = jnp.dot(hot.astype(BF16), earlier.astype(BF16), preferred_element_type=F32)
    assign = jnp.where(before == (row % SLOT).astype(F32), hot, 0.0)
    small[1].wait()
    tok = tokens_here[...]
    chosen = jnp.dot(assign.astype(BF16), tok, preferred_element_type=F32)
    for e in range(RING):
        for half in range(2):
            tx[e * 2 + half] = chosen[
                e * SLOT : (e + 1) * SLOT, half * LANES : (half + 1) * LANES
            ].astype(BF16)
    me_x = x * 2 + core
    rx[me_x] = tx[me_x]

    pl.semaphore_wait(barrier, 4 * (RING - 1) + 1)

    for d in (4, 3, 5, 2, 6, 1, 7, 0):
        e = (x + d) % RING
        send(tx.at[e * 2 + 1 - core], rx.at[me_x], x_send, x_recv, device(e, y, z, 1 - core))
        if d:
            send(tx.at[e * 2 + core], rx.at[me_x], x_send, x_recv, device(e, y, z, core))

    partner = device(x, y, z, 1 - core)
    units = pl.ds(pl.multiple_of(core * LANES, LANES), LANES)

    def down_columns(block, half):
        return down.at[:, pl.ds(pl.multiple_of((block * 2 + half) * LANES, LANES), LANES)]

    @pl.loop(0, 2 * RING)
    def _(block):
        high, wy = block // RING, block % RING
        for half in range(2):
            place = block if half == 0 else wy * 2 + high
            if half == 0:
                down_place = wd_z.at[high, units, pl.ds(pl.multiple_of(wy * LANES, LANES), LANES)]
            else:
                down_place = wd_y.at[wy, units, pl.ds(pl.multiple_of(high * LANES, LANES), LANES)]
            moves = (
                (gate.at[block, half], wg.at[place, :, units]),
                (up.at[block, half], wu.at[place, :, units]),
                (down_columns(block, half), down_place),
            )

            @pl.when(core == half)
            def _(moves=moves):
                for i, (src, dst) in enumerate(moves):
                    pltpu.make_async_copy(src, dst, weight_local.at[i]).start()

            @pl.when(core != half)
            def _(moves=moves):
                for i, (src, dst) in enumerate(moves):
                    send(src, dst, weight_send.at[i], weight_recv.at[i], partner)

    own_lanes = iota((RING, LANES), 1) % RING == iota((RING, LANES), 0)
    of_token = jnp.where(iota((TOK, LANES), 1) // RING == iota((TOK, LANES), 0), 1.0, 0.0)
    small[2].wait()
    term = lax.dot_general(router_here[...], tok, (((1,), (1,)), ((), ())), preferred_element_type=F32)
    wide = jnp.dot(term, of_token, precision=lax.Precision.HIGHEST, preferred_element_type=F32)
    logit_y[0] = jnp.sum(jnp.where(own_lanes, wide, 0.0), axis=0, keepdims=True)
    for d in (4, 3, 5, 2, 6, 1, 7):
        send(logit_y.at[0], logit_y.at[d], logit_send.at[0], logit_recv.at[0], device(x, (y + d) % RING, z, core))
    acc[...] = jnp.zeros_like(acc)
    packed = jnp.where(
        iota((ROWS, LANES), 1) == (iota((ROWS, LANES), 0) // CAP) * SLOT + iota((ROWS, LANES), 0) % CAP, 1.0, 0.0
    ).astype(BF16)

    wait(rx.at[pl.ds(0, 15)], x_recv)
    arrived = rx[...].astype(F32).reshape(2 * RING * SLOT, LANES).astype(BF16)
    xg[0, a1] = jnp.dot(packed, arrived, preferred_element_type=F32).astype(BF16)
    for d in (1, 7, 2, 6, 3, 5, 4):
        send(xg.at[0, a1], xg.at[0, a1], first_send, first_recv.at[a1], on_plane((a1 + d) % RING, a2))

    def along(d2, j, to, hop, sem):
        send(xg.at[d2, j], xg.at[to, j], ring_send, sem, on_plane(a1, (a2 + hop + RING) % RING))

    def to_second(j):
        along(0, j, 2, 2, pair_recv.at[j])
        along(0, j, 6, -2, pair_recv.at[j])

    def to_next(j):
        along(0, j, 1, 1, batch_recv.at[1])
        along(0, j, 7, -1, batch_recv.at[7])

    def from_second(j):
        wait(xg.at[pl.ds(0, 2), j], pair_recv.at[j])
        for i, (at, sign) in enumerate(((2, 1), (6, -1))):

            @pl.when(j % 2 == i)
            def _(at=at, sign=sign):
                along(at, j, 4, 2 * sign, batch_recv.at[4])

            along(at, j, at + sign, sign, batch_recv.at[at + sign])

    def multiply(d2):
        origin = (a2 + RING - d2) % RING

        @pl.when(core == 0)
        def _():
            rows = jnp.concatenate([xg[d2, j] for j in range(RING)], axis=1)
            group, first = origin % 4, (origin // 4) * RING
            for i, w in enumerate((wg, wu)):
                acc[group, i] += jnp.dot(
                    rows, w[pl.ds(first, RING)].reshape(RING * LANES, 2 * LANES), preferred_element_type=F32
                )

        @pl.when(core == 1)
        def _():
            rows = jnp.concatenate(
                [xg[d2, 0:4].reshape(4 * ROWS, LANES), xg[d2, 4:8].reshape(4 * ROWS, LANES)], axis=1
            )
            for i, w in enumerate((wg, wu)):
                acc[:, i] += jnp.dot(
                    rows, w[pl.ds(origin * 2, 2)].reshape(2 * LANES, 2 * LANES), preferred_element_type=F32
                ).reshape(4, ROWS, 2 * LANES)

    def first_event(k):
        j = near_first(k)
        wait(xg.at[0, j], first_recv.at[j])
        to_second(j)

    to_second(a1)
    to_next(a1)
    first_event(1)
    first_event(2)
    from_second(a1)

    @pl.loop(3, RING)
    def _(k):
        first_event(k)

    @pl.loop(1, RING)
    def _(k):
        to_next(near_first(k))

    for i in range(2):
        wait(wg.at[pl.ds(0, 8)], (weight_local, weight_recv)[i].at[0])
        wait(wu.at[pl.ds(0, 8)], (weight_local, weight_recv)[i].at[1])
    multiply(0)

    @pl.loop(1, RING)
    def _(k):
        from_second(near_first(k))

    def swap(g):
        send(acc.at[g], peer.at[g], swap_send, swap_recv.at[g], partner)

    def swap_done(d2):
        @pl.when(core == 0)
        def _():
            swap((a2 + RING - d2) % 4)

    multiply(2)
    multiply(6)
    swap_done(2)
    for d2 in (1, 7, 3, 5, 4):
        wait(xg.at[d2], batch_recv.at[d2])
        multiply(d2)
        if d2 in (3, 5, 4):
            swap_done(d2)

    @pl.when(core == 1)
    def _():
        for g in range(4):
            swap(g)

    wait(logit_y.at[pl.ds(0, 7)], logit_recv.at[0])
    logit_z[...] = jnp.sum(logit_y[...], axis=0)
    send(logit_z, logit_far, logit_send.at[1], logit_recv.at[1], device(x, y, (z + 4) % RING, core))
    for i in range(2):
        wait(wd_z.at[0], (weight_local, weight_recv)[i].at[2])

    for g in range(4):
        wait(peer.at[g], swap_recv.at[g])
        by_gate = acc[g, 0] + peer[g, 0]
        by_up = acc[g, 1] + peer[g, 1]
        hid[g] = (by_gate / (1.0 + jnp.exp(-by_gate)) * by_up).astype(BF16)

    def partial(d2, put):
        target = (a2 + d2 + RING) % RING

        @pl.when(core == 0)
        def _():
            terms = jnp.dot(hid[target % 4], wd_z[target // 4], preferred_element_type=F32)
            for j in range(RING):
                put(j, terms[:, j * LANES : (j + 1) * LANES])

        @pl.when(core == 1)
        def _():
            terms = jnp.dot(hid[...].reshape(4 * ROWS, 2 * LANES), wd_y[target], preferred_element_type=F32)
            for j in range(RING):
                low, high = j % 4, j // 4
                put(j, terms[low * ROWS : (low + 1) * ROWS, high * LANES : (high + 1) * LANES])

    def hop_on(m, j, hop):
        send(
            reduce_out.at[m, j], reduce_in.at[m, j], reduce_send, reduce_recv.at[m // 3 - m // 6, j],
            on_plane(a1, (a2 + hop + RING) % RING),
        )

    def put_out(m):
        def put(j, value):
            reduce_out[m, j] = value.astype(BF16)

        return put

    def put_part(i):
        def put(j, value):
            part[i, j] = value

        return put

    partial(4, put_out(0))

    @pl.loop(0, RING)
    def _(k):
        j = far_first(k)
        hop_on(0, j, 2 - 4 * (j % 2))

    for m, d2, hop in ((1, 3, 1), (2, -3, -1), (3, 1, 1), (4, -1, -1)):
        partial(d2, put_out(m))

        @pl.loop(0, RING)
        def _(k, m=m, hop=hop):
            hop_on(m, far_first(k), hop)

    partial(2, put_part(0))
    partial(-2, put_part(1))

    @pl.loop(0, RING)
    def _(k):
        j = far_first(k)
        wait(reduce_in.at[pl.ds(0, 3), j], reduce_recv.at[0, j])
        fourth = reduce_in[0, j].astype(F32)
        even = j % 2 == 0
        ahead = part[0, j] + reduce_in[1, j].astype(F32) + jnp.where(even, fourth, 0.0)
        behind = part[1, j] + reduce_in[2, j].astype(F32) + jnp.where(even, 0.0, fourth)
        reduce_out[5, j] = ahead.astype(BF16)
        hop_on(5, j, 2)
        reduce_out[6, j] = behind.astype(BF16)
        hop_on(6, j, -2)

    partial(0, put_part(2))

    def reduced(j):
        total = part[2, j]
        wait(reduce_in.at[pl.ds(3, 4), j], reduce_recv.at[1, j])
        for m in range(3, 7):
            total += reduce_in[m, j].astype(F32)
        return total

    @pl.loop(0, RING - 1)
    def _(k):
        j = far_first(k)
        last_out[j] = reduced(j).astype(BF16)
        send(last_out.at[j], last_in.at[a1], last_send, last_recv, on_plane(j, a2))

    fin[...] = reduced(a1)

    wait(logit_far, logit_recv.at[1])
    logits = jnp.where(own_lanes, logit_z[...] + logit_far[...], 0.0)
    logits = lax.dot_general(
        logits, of_token, (((1,), (1,)), ((), ())), precision=lax.Precision.HIGHEST, preferred_element_type=F32
    )
    expert = iota((RING, TOK), 0)
    gap = jnp.sum(jnp.where(r0 == expert, logits, 0.0) - jnp.where(r1 == expert, logits, 0.0), axis=0, keepdims=True)
    combine = assign * jnp.where(hot0, 1.0 / (1.0 + jnp.exp(-gap)), 1.0 / (1.0 + jnp.exp(gap)))
    unpacked = jnp.where(
        iota((LANES, ROWS), 0) == (iota((LANES, ROWS), 1) // CAP) * SLOT + iota((LANES, ROWS), 1) % CAP, 1.0, 0.0
    ).astype(BF16)

    total = fin[...]
    wait(last_in.at[pl.ds(0, 7)], last_recv)
    for d in range(1, RING):
        total += last_in[(a1 + d) % RING].astype(F32)

    opened = jnp.dot(unpacked, total.astype(BF16), preferred_element_type=F32)
    for i in range(2 * RING):
        back_out[i] = opened[i * SLOT : (i + 1) * SLOT].astype(BF16)
    for d in (4, 3, 5, 2, 6, 1, 7, 0):
        i = (x + d) % RING
        send(back_out.at[i * 2 + 1 - core], back_in.at[core, x], back_send, back_recv, device(i, y, z, 1 - core))
        if d:
            send(back_out.at[i * 2 + core], back_in.at[core, x], back_send, back_recv, device(i, y, z, core))
    back_in[core, x] = back_out[me_x]

    wait(tx.at[pl.ds(0, 15)], x_send)
    wait(logit_y.at[pl.ds(0, 7)], logit_send.at[0])
    wait(logit_z, logit_send.at[1])
    wait(wg.at[pl.ds(0, 8)], weight_send.at[0])
    wait(wu.at[pl.ds(0, 8)], weight_send.at[1])
    wait(wd_z.at[0], weight_send.at[2])
    wait(xg.at[0, pl.ds(0, 7)], first_send)
    wait(xg.at[pl.ds(0, 7)], ring_send)
    wait(acc, swap_send)
    wait(reduce_out, reduce_send)
    wait(last_out.at[pl.ds(0, 7)], last_send)

    wait(back_out.at[pl.ds(0, 15)], back_recv)
    for half in range(2):
        pieces = back_in[half].astype(F32).reshape(RING * SLOT, LANES)
        out[:, half * LANES : (half + 1) * LANES] = lax.dot_general(
            combine, pieces, (((0,), (0,)), ((), ())), precision=lax.Precision.HIGHEST, preferred_element_type=F32
        ).astype(BF16)
    wait(back_out.at[pl.ds(0, 15)], back_send)


def per_device(tokens, routes, router_weight, gate_weight, up_weight, down_weight):
    blocks, width = 2 * RING, 2 * LANES
    dma = pltpu.SemaphoreType.DMA
    vmem = pltpu.VMEM
    in_vmem = pl.BlockSpec(memory_space=pltpu.VMEM)
    in_hbm = pl.BlockSpec(memory_space=pltpu.HBM)
    return pl.pallas_call(
        kernel,
        out_shape=jax.ShapeDtypeStruct((TOK, width), BF16),
        in_specs=[in_hbm] * 6,
        out_specs=in_vmem,
        scratch_shapes=[
            vmem((blocks, SLOT, LANES), BF16),
            vmem((blocks, SLOT, LANES), BF16),
            vmem((RING, RING, ROWS, LANES), BF16),
            vmem((blocks, LANES, width), BF16),
            vmem((blocks, LANES, width), BF16),
            vmem((2, width, RING * LANES), BF16),
            vmem((RING, width, width), BF16),
            vmem((4, 2, ROWS, width), F32),
            vmem((4, 2, ROWS, width), F32),
            vmem((4, ROWS, width), BF16),
            vmem((3, RING, ROWS, LANES), F32),
            vmem((7, RING, ROWS, LANES), BF16),
            vmem((7, RING, ROWS, LANES), BF16),
            vmem((RING, ROWS, LANES), BF16),
            vmem((RING, ROWS, LANES), BF16),
            vmem((blocks, SLOT, LANES), BF16),
            vmem((2, RING, SLOT, LANES), BF16),
            vmem((ROWS, LANES), F32),
            vmem((TOK, width), BF16),
            vmem((2, TOK), jnp.int32),
            vmem((RING, width), BF16),
            vmem((RING, 1, LANES), F32),
            vmem((1, LANES), F32),
            vmem((1, LANES), F32),
            dma((6,)),
            dma((3,)),
            dma((3,)),
            dma,
            dma,
            dma,
            dma((RING,)),
            dma,
            dma((RING,)),
            dma((RING,)),
            dma((2,)),
            dma((2,)),
            dma,
            dma((4,)),
            dma,
            dma((2, RING)),
            dma,
            dma,
            dma,
            dma,
        ],
        compiler_params=pltpu.CompilerParams(collective_id=0, has_side_effects=True, vmem_limit_bytes=40 * 2**20),
        name="moe",
    )(
        *(
            pltpu.with_memory_space_constraint(w, pltpu.HBM)
            for w in (
                tokens,
                routes.T,
                router_weight.T,
                gate_weight.reshape(blocks, 2, LANES, LANES),
                up_weight.reshape(blocks, 2, LANES, LANES),
                down_weight[0],
            )
        ),
    )


def solution(mesh):
    return jax.shard_map(
        per_device,
        mesh=mesh,
        in_specs=(
            P(("expert", "dp"), "mp"),
            P(("expert", "dp"), None),
            P("mp", None),
            P("expert", None, ("dp", "mp")),
            P("expert", None, ("dp", "mp")),
            P("expert", ("dp", "mp"), None),
        ),
        out_specs=P(("expert", "dp"), "mp"),
        check_vma=False,
    )
```
